32 devices in a mesh: row: 4 (over y, core), col: 8 (over z, x).
Axes of the slice: x: 2, y: 2, z: 4, core: 2. Of those that a mesh axis runs over, the one named last changes fastest.
Arguments:
- tokens: bfloat16 [8, 1024, 2560], P('col', 'row'), may hold values from -12 to 12
- cotangent: bfloat16 [8, 1024, 2560], P('col', 'row'), may hold values from -6 to 6
- lengths: int32 [8, 1], P('col'), may hold values from 128 to 1024, as said below
- query_down: bfloat16 [2560, 768], P(('row', 'col')), may hold values from -0.125 to 0.125
- keyval_down: bfloat16 [2560, 288], P(('row', 'col')), may hold values from -0.125 to 0.125
- query_up: bfloat16 [768, 3840], P('col', 'row'), may hold values from -0.21875 to 0.21875
- keyval_up: bfloat16 [256, 5120], P('col', 'row'), may hold values from -0.375 to 0.375
- out_weight: bfloat16 [2560, 2560], P('row', 'col'), may hold values from -2.5 to 2.5
- gate_weight: bfloat16 [2560, 6400], P('col', 'row'), may hold values from -0.125 to 0.125
- up_weight: bfloat16 [2560, 6400], P('col', 'row'), may hold values from -0.125 to 0.125
- down_weight: bfloat16 [6400, 2560], P('row', 'col'), may hold values from -0.875 to 0.875
- attention_gain: float32 [2560], replicated, may hold values from 0.1 to 1.9
- feed_gain: float32 [2560], replicated, may hold values from 0.1 to 1.9
- query_gain: float32 [768], replicated, may hold values from 0.1 to 1.9
- latent_gain: float32 [256], replicated, may hold values from 0.1 to 1.9
Outputs:
- output: bfloat16 [8, 1024, 2560], P('col', 'row')
- input_grad: bfloat16 [8, 1024, 2560], P('col', 'row')
- query_down_grad: float32 [2560, 768], P(('row', 'col'))
- keyval_down_grad: float32 [2560, 288], P(('row', 'col'))
- query_up_grad: float32 [768, 3840], P('col', 'row')
- keyval_up_grad: float32 [256, 5120], P('col', 'row')
- out_weight_grad: float32 [2560, 2560], P('row', 'col')
- gate_weight_grad: float32 [2560, 6400], P('col', 'row')
- up_weight_grad: float32 [2560, 6400], P('col', 'row')
- down_weight_grad: float32 [6400, 2560], P('row', 'col')
- attention_gain_grad: float32 [2560], P(('row', 'col'))
- feed_gain_grad: float32 [2560], P(('row', 'col'))
- query_gain_grad: float32 [768], P(('row', 'col'))
- latent_gain_grad: float32 [256], P(('row', 'col'))
- root_means: float32 [3], replicated
The draws below stay inside these ranges and needn't reach their ends.
Inputs may be any that keep to these rules, and one draw needn't show every extreme that they name: `lengths`: at least one sequence has all 1024 positions valid.
All inputs are finite; a program needn't handle non-finite values.
Results may differ from the reference program's by a relative error of at most 0.018.
Values may be sent and summed in bfloat16 or wider, within the bound.
A program may use at most 256 MiB of HBM per device.

```python
import math
import jax
import jax.numpy as jnp
from jax import lax

D = 2560
H = 40
HN = 64
R = 32
V = 64
QR = 768
KVR = 256
FF = 6400
SEQLEN = 1024
GROUP_TOK = 1024
GROUPS = 8
SEQ_GRP = 1


def draw_lengths(key, part):
    first_key, second_key = jax.random.split(key)
    seq_total = GROUPS * SEQ_GRP
    drawn_len = jax.random.randint(first_key, (seq_total,), SEQLEN // 8, SEQLEN + 1)
    chosen = jax.random.randint(second_key, (), 0, seq_total)
    drawn_len = jnp.where(jnp.arange(seq_total) == chosen, SEQLEN, drawn_len)
    return drawn_len.reshape(GROUPS, SEQ_GRP).astype(jnp.int32)


def draw_tokens(key, part):
    base_key, column_key = jax.random.split(key, 2)
    shape_all = (GROUPS, GROUP_TOK, D)
    row_scale = 0.4 + 1.2 * jnp.arange(GROUP_TOK, dtype=jnp.float32) / GROUP_TOK
    column_scale = jnp.exp(jax.random.uniform(column_key, (D,), jnp.float32, -0.8, 0.8))
    base_draw = jnp.clip(jax.random.normal(base_key, shape_all, jnp.float32), -4.0, 4.0)
    return jnp.clip(base_draw * row_scale[None, :, None] * column_scale[None, None, :], -12.0, 12.0).astype(jnp.bfloat16)


def level_of(key, extent, cuts, smallest, largest):
    def one(axis_at, shards_of):
        heights = jax.random.uniform(jax.random.fold_in(jax.random.fold_in(key, 6), axis_at), (shards_of,), jnp.float32, smallest / len(cuts), largest / len(cuts))
        return jnp.repeat(jnp.exp(heights), extent[axis_at] // shards_of).reshape((-1,) + (1,) * (len(extent) - axis_at - 1))

    loudness = one(*cuts[0])
    for cut in cuts[1:]:
        loudness = loudness * one(*cut)
    return loudness


def bell_draw(rng, extent, scale, bound, cuts=(), kind=jnp.bfloat16):
    loudness = level_of(rng, extent, cuts, -0.22, 0.18) if cuts else 1.0
    values = jax.random.normal(rng, extent, jnp.float32) * scale * loudness
    return jnp.minimum(jnp.maximum(values, -bound), bound).astype(kind)


def setup_inputs(seed: int = 0) -> dict:
    key_list = jax.random.split(jax.random.key(seed), 16)
    return {
        "tokens": draw_tokens(jax.random.fold_in(key_list[15], 71), 0),
        "cotangent": bell_draw(key_list[1], (GROUPS, GROUP_TOK, D), 1.0, 6.0, ((0, 8), (1, 4))),
        "lengths": draw_lengths(jax.random.fold_in(key_list[15], 71), 0),
        "query_down": bell_draw(key_list[3], (D, QR), D ** -0.5, 0.125, ((0, 32),)),
        "keyval_down": bell_draw(key_list[4], (D, KVR + R), D ** -0.5, 0.125, ((0, 32),)),
        "query_up": bell_draw(key_list[5], (QR, H * (HN + R)), QR ** -0.5, 0.21875, ((0, 8), (1, 4))),
        "keyval_up": bell_draw(key_list[6], (KVR, H * (HN + V)), KVR ** -0.5, 0.375, ((0, 8), (1, 4))),
        "out_weight": bell_draw(key_list[7], (H * V, D), (max(1, H * V // 512)) ** -0.5, 2.5, ((0, 4), (1, 8))),
        "gate_weight": bell_draw(key_list[8], (D, FF), D ** -0.5, 0.125, ((0, 8), (1, 4))),
        "up_weight": bell_draw(key_list[9], (D, FF), D ** -0.5, 0.125, ((0, 8), (1, 4))),
        "down_weight": bell_draw(key_list[10], (FF, D), (max(1, FF // 128)) ** -0.5, 0.875, ((0, 4), (1, 8))),
        "attention_gain": jnp.clip(1.0 + 0.18 * jax.random.normal(key_list[11], (D,), jnp.float32), 0.1, 1.9),
        "feed_gain": jnp.clip(1.0 + 0.18 * jax.random.normal(key_list[12], (D,), jnp.float32), 0.1, 1.9),
        "query_gain": jnp.clip(1.0 + 0.18 * jax.random.normal(key_list[13], (QR,), jnp.float32), 0.1, 1.9),
        "latent_gain": jnp.clip(1.0 + 0.18 * jax.random.normal(key_list[14], (KVR,), jnp.float32), 0.1, 1.9),
    }


@jax.custom_vjp
def low(v):
    return lax.optimization_barrier(v.astype(jnp.bfloat16)).astype(jnp.float32)

@jax.custom_vjp
def low_back(v):
    return v

def low_keep(v):
    return (low(v), None)

def low_pass(kept, grad):
    return (grad,)

def back_keep(v):
    return (v, None)

def back_low(kept, grad):
    return (low(grad),)
low.defvjp(low_keep, low_pass)
low_back.defvjp(back_keep, back_low)
highest = lax.Precision.HIGHEST
eps = 1e-05
branch_scale = 1.4 / math.sqrt(62.0)
masked_fill = -1e+30

def product(left_arr, right_arr):
    return jnp.dot(left_arr, right_arr, precision=highest)

def root_norm(values, gain_vec):
    return values * lax.rsqrt(lax.optimization_barrier(jnp.mean(values * values, axis=-1, keepdims=True)) + eps) * gain_vec

def rotate(values, positions):
    half_dim = values.shape[-1] // 2
    frequency = jnp.exp(jnp.arange(half_dim, dtype=jnp.float32) * (-2.0 * math.log(10000.0) / values.shape[-1]))
    angles = positions.astype(jnp.float32)[:, None] * frequency[None, :]
    target = (values.shape[0],) + (1,) * (values.ndim - 2) + (half_dim,)
    cosine = jnp.cos(angles).reshape(target)
    sine_val = jnp.sin(angles).reshape(target)
    first_half = values[..., :half_dim]
    second_half = values[..., half_dim:]
    return jnp.concatenate([first_half * cosine - second_half * sine_val, second_half * cosine + first_half * sine_val], axis=-1)

def silu_product(gate_act, up_act):
    return gate_act * lax.logistic(gate_act) * up_act

def attend_one(query_rows, key_nope, key_rope, value_rows, length):
    seq_span = query_rows.shape[0]
    raw_scores = jnp.einsum('qhd,khd->hqk', query_rows[..., :HN], key_nope, precision=highest)
    raw_scores = raw_scores + jnp.einsum('qhd,kd->hqk', query_rows[..., HN:], key_rope, precision=highest)
    scores = low_back(raw_scores) * (1.0 / math.sqrt(HN + R))
    places = jnp.arange(seq_span, dtype=jnp.int32)
    allowed = (places[None, :] <= places[:, None]) & (places[None, :] < length)
    scores = jnp.where(allowed[None], scores, masked_fill)
    row_max = lax.optimization_barrier(jnp.max(scores, axis=-1, keepdims=True))
    weights = jnp.exp(scores - row_max)
    softmax = weights / lax.optimization_barrier(jnp.sum(weights, axis=-1, keepdims=True))
    return jnp.einsum('hqk,khd->qhd', low(softmax), value_rows, precision=highest)

def forward_layer(inputs, seq_lengths, query_down, keyval_down, query_up, keyval_up, out_weight, gate_weight, up_weight, down_weight, attention_gain, feed_gain, query_gain, latent_gain):
    row_total = inputs.shape[0]
    positions = jnp.arange(row_total, dtype=jnp.int32) % SEQLEN
    normed = low(root_norm(inputs, attention_gain))
    query_lat_raw = low_back(product(normed, query_down))
    keyval_raw = low_back(product(normed, keyval_down))
    query_latent = low(root_norm(query_lat_raw, query_gain))
    keyval_latent = low(root_norm(keyval_raw[:, :KVR], latent_gain))
    key_rope = low(rotate(keyval_raw[:, KVR:], positions))
    query_raw = low_back(product(query_latent, query_up)).reshape(row_total, H, HN + R)
    queries = low(jnp.concatenate([query_raw[..., :HN], rotate(query_raw[..., HN:], positions)], axis=-1))
    keyvals = low(low_back(product(keyval_latent, keyval_up))).reshape(row_total, H, HN + V)
    seq_count = row_total // SEQLEN

    def attend_seq(seq_items):
        return jax.checkpoint(attend_one)(*seq_items)
    attended = lax.map(attend_seq, (queries.reshape(seq_count, SEQLEN, H, HN + R), keyvals[..., :HN].reshape(seq_count, SEQLEN, H, HN), key_rope.reshape(seq_count, SEQLEN, R), keyvals[..., HN:].reshape(seq_count, SEQLEN, H, V), seq_lengths))
    attn_vals = low(low_back(attended.reshape(row_total, H * V)))
    attn_out = low_back(product(attn_vals, out_weight))
    residual = inputs + branch_scale * attn_out
    normed_two = low(root_norm(residual, feed_gain))
    gate_act = low_back(product(normed_two, gate_weight))
    up_act = low_back(product(normed_two, up_weight))
    hidden = low(silu_product(gate_act, up_act))
    feed_out = low_back(product(hidden, down_weight))
    return (residual + branch_scale * feed_out, (attn_out, feed_out))

def reference(tokens, cotangent, lengths, query_down, keyval_down, query_up, keyval_up, out_weight, gate_weight, up_weight, down_weight, attention_gain, feed_gain, query_gain, latent_gain):
    flat_rows = tokens.reshape(-1, D).astype(jnp.float32)
    seq_lengths = lengths.reshape(-1).astype(jnp.int32)
    row_ids = jnp.arange(flat_rows.shape[0], dtype=jnp.int32)
    seq_ids = row_ids // SEQLEN
    valid_rows = (row_ids % SEQLEN < seq_lengths[seq_ids]).astype(jnp.float32)[:, None]
    params = tuple((weight_arr.astype(jnp.float32) for weight_arr in (query_down, keyval_down, query_up, keyval_up, out_weight, gate_weight, up_weight, down_weight, attention_gain, feed_gain, query_gain, latent_gain)))

    def closed(inputs, *weights):
        return forward_layer(inputs, seq_lengths, *weights)
    result, pullback, extras = jax.vjp(closed, flat_rows, *params, has_aux=True)
    attn_out, feed_out = extras
    gradients = pullback(cotangent.reshape(-1, D).astype(jnp.float32) * valid_rows)
    valid_total = jnp.sum(valid_rows) * D
    root_means = jnp.stack([jnp.sqrt(jnp.sum(result * result * valid_rows) / valid_total), jnp.sqrt(jnp.sum(attn_out * attn_out * valid_rows) / valid_total), jnp.sqrt(jnp.sum(feed_out * feed_out * valid_rows) / valid_total)])
    return (result.astype(jnp.bfloat16).reshape(tokens.shape), gradients[0].astype(jnp.bfloat16).reshape(tokens.shape), gradients[1], gradients[2], gradients[3], gradients[4], gradients[5], gradients[6], gradients[7], gradients[8], gradients[9], gradients[10], gradients[11], gradients[12], root_means)
```

```python
import functools
import math

import jax
import jax.numpy as jnp
from jax import lax
from jax.experimental import pallas as pl
from jax.experimental.pallas import tpu as pltpu
from jax.sharding import PartitionSpec as P

D = 2560
HN = 64
R = 32
V = 64
QR = 768
KVR = 256
SEQLEN = 1024
QB = 256

eps = 1e-05
branch_scale = 1.4 / math.sqrt(62.0)
masked_fill = -1e30
scaling = 1.0 / math.sqrt(HN + R)
LOG2E = math.log2(math.e)


bf16 = jnp.bfloat16
f32 = jnp.float32


def dot(left_arr, right_arr, left_dim, right_dim):
    return lax.dot_general(
        left_arr, right_arr, (((left_dim,), (right_dim,)), ((), ())), preferred_element_type=f32
    )


def norm_scale(values):
    return lax.rsqrt(jnp.mean(values * values, axis=-1, keepdims=True) + eps)


def root_norm(values, gain_vec):
    return values * norm_scale(values) * gain_vec


def norm_back(values, gain_vec, grads):
    scale = norm_scale(values)
    weighted = grads * gain_vec
    inner = jnp.mean(weighted * values, axis=-1, keepdims=True)
    d_values = scale * weighted - values * (scale * scale * scale) * inner
    d_gain = jnp.sum(grads * values * scale, axis=0)
    return d_values, d_gain


def rope_tables(positions):
    frequency = jnp.exp(
        jnp.arange(R // 2, dtype=f32) * (-2.0 * math.log(10000.0) / R)
    )
    angles = positions.astype(f32)[:, None] * frequency[None, :]
    return jnp.cos(angles), jnp.sin(angles)


def rotate(values, cosine, sine):
    first, second = values[:, : R // 2], values[:, R // 2 :]
    return jnp.concatenate(
        [first * cosine - second * sine, second * cosine + first * sine], axis=1
    )


def head_scores(key_rows, query_cols, start, limit):
    span = key_rows.shape[0]
    raw = jnp.dot(key_rows, query_cols, preferred_element_type=f32) * (scaling * LOG2E)
    keys = lax.broadcasted_iota(jnp.int32, (span, QB), 0)
    bound = jnp.minimum(lax.broadcasted_iota(jnp.int32, (1, QB), 1) + (start + 1), limit)
    return jnp.where(keys < bound, raw, masked_fill)


def forward_kernel(len_ref, q_ref, kv_ref, kpe_ref, out_ref, lse_ref):
    limit = len_ref[pl.program_id(0)]
    kv = kv_ref[...]
    value_t = kv.T[HN:]
    key_rows = jnp.concatenate([kv[:, :HN], kpe_ref[...]], axis=1)
    for block in range(SEQLEN // QB):
        start, span = block * QB, (block + 1) * QB
        scores = head_scores(key_rows[:span], q_ref[:, start:span], start, limit)
        row_max = jnp.max(scores, axis=0, keepdims=True)
        weights = jnp.exp2(scores - row_max)
        total = jnp.sum(weights, axis=0, keepdims=True)
        probs = (weights * (1.0 / total)).astype(bf16)
        mixed = jnp.dot(value_t[:, :span], probs, preferred_element_type=f32)
        out_ref[:, start:span] = mixed.astype(bf16)
        lse_ref[0, :, start:span] = row_max + jnp.log2(total)


def backward_kernel(
    len_ref, q_ref, kv_ref, kpe_ref, g_ref, lse_ref, cos_ref, sin_ref,
    dq_ref, dkv_ref, dkpe_ref, dk_acc, dv_acc,
):
    limit = len_ref[pl.program_id(0)]
    kv = kv_ref[...]
    key_rows = jnp.concatenate([kv[:, :HN], kpe_ref[...]], axis=1)
    key_t = key_rows.T
    value_rows = kv[:, HN:]
    query_rows = q_ref[...].T
    grad_rows = g_ref[...].T
    for block in reversed(range(SEQLEN // QB)):
        start, span = block * QB, (block + 1) * QB
        scores = head_scores(key_rows[:span], q_ref[:, start:span], start, limit)
        probs = jnp.exp2(scores - lse_ref[0, :, start:span])
        g_probs = jnp.dot(value_rows[:span], g_ref[:, start:span], preferred_element_type=f32)
        centre = jnp.sum(probs * g_probs, axis=0, keepdims=True)
        g_scores = (probs * (g_probs - centre) * scaling).astype(bf16)
        d_query = jnp.dot(key_t[:, :span], g_scores, preferred_element_type=f32)
        first, second = d_query[HN : HN + R // 2], d_query[HN + R // 2 :]
        cosine, sine = cos_ref[:, start:span], sin_ref[:, start:span]
        dq_ref[:HN, start:span] = d_query[:HN].astype(bf16)
        dq_ref[HN : HN + R // 2, start:span] = (first * cosine + second * sine).astype(bf16)
        dq_ref[HN + R // 2 :, start:span] = (second * cosine - first * sine).astype(bf16)
        dk = jnp.dot(g_scores, query_rows[start:span], preferred_element_type=f32)
        dv = jnp.dot(probs.astype(bf16), grad_rows[start:span], preferred_element_type=f32)
        if span == SEQLEN:
            dk_acc[...] = dk
            dv_acc[...] = dv
        else:
            dk_acc[:span] += dk
            dv_acc[:span] += dv
    dk = dk_acc[...]
    dkv_ref[...] = jnp.concatenate([dk[:, :HN], dv_acc[...]], axis=1).astype(bf16)

    @pl.when(pl.program_id(1) == 0)
    def _():
        dkpe_ref[...] = dk[:, HN:]

    @pl.when(pl.program_id(1) != 0)
    def _():
        dkpe_ref[...] += dk[:, HN:]


def head_specs():
    return [
        pl.BlockSpec(memory_space=pltpu.SMEM),
        pl.BlockSpec((HN + R, SEQLEN), lambda s, h: (h, s)),
        pl.BlockSpec((SEQLEN, HN + V), lambda s, h: (s, h)),
        pl.BlockSpec((SEQLEN, R), lambda s, h: (s, 0)),
    ]


def attention_forward(lengths, q_t, kv, k_pe):
    rows = kv.shape[0]
    heads = kv.shape[1] // (HN + V)
    cells = heads * rows * SEQLEN
    return pl.pallas_call(
        forward_kernel,
        grid=(rows // SEQLEN, heads),
        in_specs=head_specs(),
        out_specs=[
            pl.BlockSpec((V, SEQLEN), lambda s, h: (h, s)),
            pl.BlockSpec((1, 1, SEQLEN), lambda s, h: (h, 0, s)),
        ],
        out_shape=[
            jax.ShapeDtypeStruct((heads * V, rows), bf16),
            jax.ShapeDtypeStruct((heads, 1, rows), f32),
        ],
        cost_estimate=pl.CostEstimate(
            flops=cells * 6 * 256, transcendentals=cells, bytes_accessed=rows * heads * 600
        ),
        compiler_params=pltpu.CompilerParams(vmem_limit_bytes=48 * 2**20),
        name="attn_forward",
    )(lengths, q_t, kv, k_pe)


def attention_backward(lengths, q_t, kv, k_pe, g_t, lse, cos_t, sin_t):
    rows = kv.shape[0]
    heads = kv.shape[1] // (HN + V)
    cells = heads * rows * SEQLEN
    return pl.pallas_call(
        backward_kernel,
        grid=(rows // SEQLEN, heads),
        in_specs=head_specs()
        + [
            pl.BlockSpec((V, SEQLEN), lambda s, h: (h, s)),
            pl.BlockSpec((1, 1, SEQLEN), lambda s, h: (h, 0, s)),
            pl.BlockSpec((R // 2, SEQLEN), lambda s, h: (0, s)),
            pl.BlockSpec((R // 2, SEQLEN), lambda s, h: (0, s)),
        ],
        out_specs=[
            pl.BlockSpec((HN + R, SEQLEN), lambda s, h: (h, s)),
            pl.BlockSpec((SEQLEN, HN + V), lambda s, h: (s, h)),
            pl.BlockSpec((SEQLEN, R), lambda s, h: (s, 0)),
        ],
        out_shape=[
            jax.ShapeDtypeStruct((heads * (HN + R), rows), bf16),
            jax.ShapeDtypeStruct((rows, heads * (HN + V)), bf16),
            jax.ShapeDtypeStruct((rows, R), f32),
        ],
        scratch_shapes=[
            pltpu.VMEM((SEQLEN, HN + R), f32),
            pltpu.VMEM((SEQLEN, V), f32),
        ],
        cost_estimate=pl.CostEstimate(
            flops=cells * 14 * 256, transcendentals=cells, bytes_accessed=rows * heads * 1200
        ),
        compiler_params=pltpu.CompilerParams(vmem_limit_bytes=48 * 2**20),
        name="attn_backward",
    )(lengths, q_t, kv, k_pe, g_t, lse, cos_t, sin_t)


def swap(array, axis, bit):
    size = lax.axis_size(axis)
    return lax.ppermute(array, axis, [(i, i ^ bit) for i in range(size)])


def col_bits():
    size = lax.axis_size("col")
    bits = [1 << i for i in range(size.bit_length() - 1)]
    return bits[1:] + bits[:1]


def gather_col(block):
    rows = block.shape[0]
    me = lax.axis_index("col")
    size = lax.axis_size("col")
    held = [(0, block)]
    for bit in col_bits():
        held = held + [(offset ^ bit, swap(part, "col", bit)) for offset, part in held]
    full = jnp.zeros((size * rows,) + block.shape[1:], block.dtype)
    for offset, part in held:
        full = lax.dynamic_update_slice_in_dim(full, part, (me ^ offset) * rows, 0)
    return full


def scatter_col(grads):
    size = lax.axis_size("col")
    me = lax.axis_index("col")
    n_bits = size.bit_length() - 1
    rows = grads.shape[0] // size
    parts = grads.astype(bf16).reshape((2,) * n_bits + (rows,) + grads.shape[1:])
    order = col_bits()[::-1]
    alive = sorted(order, reverse=True)
    for bit in order:
        axis = alive.index(bit)
        mine = (me // bit) % 2
        kept = lax.dynamic_index_in_dim(parts, mine, axis, keepdims=False)
        sent = lax.dynamic_index_in_dim(parts, 1 - mine, axis, keepdims=False)
        alive.remove(bit)
        parts = kept.astype(f32) + swap(sent.astype(bf16), "col", bit).astype(f32)
    return parts


def on_device(
    tokens, cotangent, lengths, query_down, keyval_down, query_up, keyval_up, out_weight,
    gate_weight, up_weight, down_weight, attention_gain, feed_gain, query_gain, latent_gain,
):
    rows_dev = tokens.shape[1]
    row_devices = lax.axis_size("row")
    row_rank = lax.axis_index("row")
    group_rows = rows_dev * row_devices
    own_start = row_rank * rows_dev
    seq_lengths = lengths[0]
    inputs = tokens[0].astype(f32)

    positions = jnp.arange(group_rows, dtype=jnp.int32) % SEQLEN
    cosine, sine = rope_tables(positions)
    own_rows = own_start + jnp.arange(rows_dev, dtype=jnp.int32)
    own_cos, own_sin = rope_tables(own_rows % SEQLEN)
    own_seq = own_rows // SEQLEN
    own_length = jnp.sum(
        jnp.where(
            own_seq[:, None] == jnp.arange(seq_lengths.shape[0])[None, :], seq_lengths[None, :], 0
        ),
        axis=1,
    )
    valid_rows = (own_rows % SEQLEN < own_length).astype(f32)[:, None]

    downs = jnp.concatenate([query_down, keyval_down], axis=1)
    downs_all = lax.all_gather(downs, ("row", "col"), axis=0, tiled=True)
    query_up_all = gather_col(query_up)
    keyval_up_all = gather_col(keyval_up)
    out_all = gather_col(out_weight.T)
    gate_all = gather_col(gate_weight)
    up_all = gather_col(up_weight)
    down_all = gather_col(down_weight.T)

    def gather_rows(values):
        return lax.all_gather(values, "row", axis=0, tiled=True)

    def scatter_rows(values):
        return lax.psum_scatter(
            values.astype(bf16), "row", scatter_dimension=0, tiled=True
        ).astype(f32)

    normed = root_norm(inputs, attention_gain).astype(bf16)
    latents = dot(normed, downs_all, 1, 0)
    query_a = latents[:, :QR]
    latent_a = latents[:, QR : QR + KVR]
    own_latents = jnp.concatenate(
        [
            root_norm(query_a, query_gain),
            root_norm(latent_a, latent_gain),
            rotate(latents[:, QR + KVR :], own_cos, own_sin),
        ],
        axis=1,
    ).astype(bf16)
    group_latents = gather_rows(own_latents)
    query_latent = group_latents[:, :QR]
    keyval_latent = group_latents[:, QR : QR + KVR]
    k_pe = group_latents[:, QR + KVR :]
    heads = keyval_up_all.shape[1] // (HN + V)
    cos_t, sin_t = cosine.T, sine.T
    raw_t = dot(query_up_all, query_latent, 0, 1).reshape(heads, HN + R, group_rows)
    first, second = raw_t[:, HN : HN + R // 2], raw_t[:, HN + R // 2 :]
    q_t = (
        jnp.concatenate(
            [raw_t[:, :HN], first * cos_t - second * sin_t, second * cos_t + first * sin_t], axis=1
        )
        .astype(bf16)
        .reshape(heads * (HN + R), group_rows)
    )
    kv = dot(keyval_latent, keyval_up_all, 1, 0).astype(bf16)
    vals_t, lse = attention_forward(seq_lengths, q_t, kv, k_pe)
    attn_out = scatter_rows(dot(vals_t, out_all, 0, 1))

    residual = inputs + branch_scale * attn_out
    normed_two = root_norm(residual, feed_gain).astype(bf16)
    two_group = gather_rows(normed_two)
    gate_act = dot(two_group, gate_all, 1, 0)
    up_act = dot(two_group, up_all, 1, 0)
    sigmoid = lax.logistic(gate_act)
    hidden = (gate_act * sigmoid * up_act).astype(bf16)
    feed_out = scatter_rows(dot(hidden, down_all, 1, 1))
    output_rows = residual + branch_scale * feed_out

    grad_rows = cotangent[0].astype(f32) * valid_rows
    grad_feed = gather_rows((branch_scale * grad_rows).astype(bf16))
    grad_down = dot(grad_feed, hidden, 0, 0)
    grad_hidden = dot(grad_feed, down_all, 1, 0)
    grad_gate_act = (
        grad_hidden * up_act * sigmoid * (1.0 + gate_act * (1.0 - sigmoid))
    ).astype(bf16)
    grad_up_act = (grad_hidden * gate_act * sigmoid).astype(bf16)
    grad_gate = dot(two_group, grad_gate_act, 0, 0)
    grad_up = dot(two_group, grad_up_act, 0, 0)
    grad_two = scatter_rows(dot(grad_gate_act, gate_all, 1, 1) + dot(grad_up_act, up_all, 1, 1))
    grad_norm_two, grad_feed_gain = norm_back(residual, feed_gain, grad_two)
    grad_resid = grad_rows + grad_norm_two

    grad_attn = gather_rows((branch_scale * grad_resid).astype(bf16))
    grad_out = dot(grad_attn, vals_t, 0, 1)
    grad_vals_t = dot(out_all, grad_attn, 0, 1).astype(bf16)
    grad_q_t, grad_kv, grad_kpe = attention_backward(
        seq_lengths, q_t, kv, k_pe, grad_vals_t, lse, cos_t, sin_t
    )
    grad_query_up = dot(query_latent, grad_q_t, 0, 1)
    grad_keyval_up = dot(keyval_latent, grad_kv, 0, 0)
    grad_latents = scatter_rows(
        jnp.concatenate(
            [
                dot(grad_q_t, query_up_all, 0, 1),
                dot(grad_kv, keyval_up_all, 1, 1),
                grad_kpe,
            ],
            axis=1,
        )
    )
    grad_query_a, grad_query_gain = norm_back(query_a, query_gain, grad_latents[:, :QR])
    grad_latent_a, grad_latent_gain = norm_back(
        latent_a, latent_gain, grad_latents[:, QR : QR + KVR]
    )
    grad_low = jnp.concatenate(
        [grad_query_a, grad_latent_a, rotate(grad_latents[:, QR + KVR :], own_cos, -own_sin)],
        axis=1,
    ).astype(bf16)
    grad_downs = dot(normed, grad_low, 0, 0)
    grad_normed = dot(grad_low, downs_all, 1, 1)
    grad_input_norm, grad_attention_gain = norm_back(inputs, attention_gain, grad_normed)
    input_grad = (grad_resid + grad_input_norm).astype(bf16)

    everywhere = ("row", "col")
    stats = lax.psum(
        (
            jnp.sum(output_rows * output_rows * valid_rows),
            jnp.sum(attn_out * attn_out * valid_rows),
            jnp.sum(feed_out * feed_out * valid_rows),
            jnp.sum(valid_rows),
        ),
        everywhere,
    )
    valid_total = stats[3] * D
    root_means = jnp.stack([jnp.sqrt(stats[i] / valid_total) for i in range(3)])

    def scatter_all(values):
        return lax.psum_scatter(values, everywhere, scatter_dimension=0, tiled=True)

    grad_downs = scatter_all(grad_downs.astype(bf16)).astype(f32)
    return (
        output_rows.astype(bf16)[None],
        input_grad[None],
        grad_downs[:, :QR],
        grad_downs[:, QR:],
        scatter_col(grad_query_up),
        scatter_col(grad_keyval_up),
        scatter_col(grad_out).T,
        scatter_col(grad_gate),
        scatter_col(grad_up),
        scatter_col(grad_down).T,
        scatter_all(grad_attention_gain),
        scatter_all(grad_feed_gain),
        scatter_all(grad_query_gain),
        scatter_all(grad_latent_gain),
        root_means,
    )


def solution(mesh):
    block = P("col", "row")
    flipped = P("row", "col")
    spread = P(("row", "col"))
    group = P("col", "row", None)
    return jax.shard_map(
        on_device,
        mesh=mesh,
        in_specs=(
            group, group, P("col", None), spread, spread,
            block, block, flipped, block, block, flipped,
            P(), P(), P(), P(),
        ),
        out_specs=(
            group, group, spread, spread,
            block, block, flipped, block, block, flipped,
            spread, spread, spread, spread, P(),
        ),
        check_vma=False,
    )
```
